32 devices in a mesh: gy: 2 (over core), gx: 16 (over z, y, x).
Axes of the slice: x: 2, y: 2, z: 4, core: 2. Of those that a mesh axis runs over, the one named last changes fastest.
Arguments:
- basis_vectors: float32 [36, 64, 128, 256], P(None, 'gx', 'gy'), may hold values from -30 to 30, as said below
- reaction: float32 [64, 128, 256], P('gx', 'gy'), may hold values from 0.5 to 3
Outputs:
- new_vectors: float32 [4, 64, 128, 256], P(None, 'gx', 'gy')
- hessenberg: float32 [40, 4], replicated
The draws below stay inside these ranges and needn't reach their ends.
Inputs may be any that keep to these rules, and one draw needn't show every extreme that they name: `basis_vectors`: under the inner product the basis vectors are nearly orthonormal.
All inputs are finite; a program needn't handle non-finite values.
Results may differ from the reference program's by a relative error of at most 0.0003.
Values sent between devices are 32-bit elements; how exact they have to be, the bound alone decides.
A program may use at most 128 MiB of HBM per device.

```python
import math
import jax
import jax.numpy as jnp
from jax import lax

KEEP = 36
STEPS = 4
BASIS = 40
NX = 64
NY = 128
NZ = 256


WIND_SPEEDS = (0.9, 0.6, 0.4)


TILT_SHARE = 0.01


MIXING_SHARE = 0.003


RAMP_FACTOR = 3.0


def stencil_drawn(values, x_ext, y_ext, z_ext, reaction):
    summed = -reaction * values
    for position, extended in enumerate((x_ext, y_ext, z_ext)):
        count = values.shape[position]
        higher = lax.slice_in_dim(extended, 3, count + 3, axis=position)
        lower_one = lax.slice_in_dim(extended, 1, count + 1, axis=position)
        lower_two = lax.slice_in_dim(extended, 0, count, axis=position)
        wind_speed = WIND_SPEEDS[position]
        summed = summed + higher + lower_one - 2.0 * values - wind_speed * (3.0 * values - 4.0 * lower_one + lower_two) * 0.5
    return summed


def apply_operator_drawn(values, reaction):
    padded = jnp.pad(values, ((2, 1), (2, 1), (2, 1)))
    return stencil_drawn(values, padded[:, 2:-1, 2:-1], padded[2:-1, :, 2:-1], padded[2:-1, 2:-1, :], reaction)


def reaction_field(key):
    key_field = jax.random.fold_in(key, 7)
    shape = (NX, NY, NZ)
    return jax.random.uniform(key_field, shape, jnp.float32, 0.5, 3.0)


def draw_reaction(key, part):
    return reaction_field(key)


def rough_fields(key, count, plane_scale):
    shape = (count, NX, NY, NZ)
    values = jax.random.normal(key, shape, jnp.float32)
    return values * plane_scale


def draw_basis_vectors(key, part):
    key_list = jax.random.split(jax.random.fold_in(key, 11), 4)
    plane_index = jnp.arange(NX, dtype=jnp.float32).reshape(NX, 1, 1)
    plane_scale = jnp.exp(math.log(RAMP_FACTOR) * plane_index / float(NX - 1))
    plane_scale = plane_scale / jnp.sqrt(jnp.mean(plane_scale * plane_scale))
    seed_fields = rough_fields(key_list[0], 2, plane_scale)
    start_field = seed_fields[0] / jnp.sqrt(jnp.mean(seed_fields[0] * seed_fields[0]))
    image_field = apply_operator_drawn(start_field, reaction_field(key))
    tilted = image_field + TILT_SHARE * jnp.sqrt(jnp.mean(image_field * image_field)) * seed_fields[1]
    tilted = tilted - jnp.sum(tilted * start_field) / jnp.sum(start_field * start_field) * start_field
    tilted = tilted / jnp.sqrt(jnp.mean(tilted * tilted))
    row_fields = jnp.concatenate([start_field[None], tilted[None], rough_fields(key_list[1], KEEP - 2, plane_scale)], axis=0)
    gram_matrix = jnp.einsum('axyz,bxyz->ab', row_fields, row_fields, precision=lax.Precision.HIGHEST) / float(NX * NY * NZ)
    inverse = jnp.linalg.inv(jnp.linalg.cholesky(gram_matrix))
    moved_order = jnp.concatenate([jnp.arange(1, KEEP, dtype=jnp.int32), jnp.zeros((1,), jnp.int32)])
    shuffle = jnp.eye(KEEP, dtype=jnp.float32)[moved_order]
    mixing = jnp.eye(KEEP, dtype=jnp.float32) + MIXING_SHARE * jax.random.normal(key_list[2], (KEEP, KEEP), jnp.float32)
    matrix = jnp.dot(mixing, jnp.dot(shuffle, inverse, precision=lax.Precision.HIGHEST), precision=lax.Precision.HIGHEST)
    return jnp.einsum('ab,bxyz->axyz', matrix, row_fields, precision=lax.Precision.HIGHEST)


def setup_inputs(seed: int = 0) -> dict:
    splits = jax.random.split(jax.random.key(seed), 3)
    basis_vectors = draw_basis_vectors(jax.random.fold_in(splits[2], 71), 0)
    reaction = draw_reaction(jax.random.fold_in(splits[2], 71), 0)
    return {"basis_vectors": basis_vectors, "reaction": reaction}


WIND_SPEEDS = (0.9, 0.6, 0.4)
EPSILON = 1e-06

def stencil(values, x_ext, y_ext, z_ext, reaction):
    summed = -reaction * values
    for position, extended in enumerate((x_ext, y_ext, z_ext)):
        count = values.shape[position]
        higher = lax.slice_in_dim(extended, 3, count + 3, axis=position)
        lower_one = lax.slice_in_dim(extended, 1, count + 1, axis=position)
        lower_two = lax.slice_in_dim(extended, 0, count, axis=position)
        wind_speed = WIND_SPEEDS[position]
        summed = summed + higher + lower_one - 2.0 * values - wind_speed * (3.0 * values - 4.0 * lower_one + lower_two) * 0.5
    return summed

def apply_operator(values, reaction):
    padded = jnp.pad(values, ((2, 1), (2, 1), (2, 1)))
    return stencil(values, padded[:, 2:-1, 2:-1], padded[2:-1, :, 2:-1], padded[2:-1, 2:-1, :], reaction)

def project(basis_vectors, created, image):
    local = jnp.einsum('kxyz,xyz->k', basis_vectors, image, precision=lax.Precision.HIGHEST)
    extra = [jnp.sum(vector * image)[None] for vector in created]
    return jnp.concatenate([local] + extra)

def combine(basis_vectors, created, weights):
    keep_count = basis_vectors.shape[0]
    summed = jnp.einsum('k,kxyz->xyz', weights[:keep_count], basis_vectors, precision=lax.Precision.HIGHEST)
    for index, vector in enumerate(created):
        summed = summed + weights[keep_count + index] * vector
    return summed

def reference(basis_vectors, reaction):
    cell_count = float(NX * NY * NZ)
    created = []
    columns = []
    for section in range(STEPS):
        current = KEEP + section
        vector_now = basis_vectors[KEEP - 1] if section == 0 else created[-1]
        image = apply_operator(vector_now, reaction)
        first_terms = project(basis_vectors, created, image) / cell_count
        first_rest = image - combine(basis_vectors, created, first_terms)
        second_terms = project(basis_vectors, created, first_rest) / cell_count
        second_rest = first_rest - combine(basis_vectors, created, second_terms)
        length_now = jnp.sqrt(jnp.sum(second_rest * second_rest) / cell_count + EPSILON)
        columns.append(jnp.concatenate([first_terms + second_terms, length_now[None], jnp.zeros((BASIS - current - 1,), jnp.float32)]))
        created.append(second_rest / length_now)
    return (jnp.stack(created), jnp.stack(columns, axis=1))
```

```python
import functools

import jax
import jax.numpy as jnp
from jax import lax
from jax.experimental import pallas as pl
from jax.experimental.pallas import tpu as pltpu
from jax.sharding import PartitionSpec as P

STEPS = 4
WIND_SPEEDS = (0.9, 0.6, 0.4)
EPSILON = 1e-06
MESH = pl.DeviceIdType.MESH
BLOCK = 6
LOADS = 6


def roll(values, shift, axis):
    return pltpu.roll(values, shift, axis)


def fold_lanes(values):
    parts = [values[:, s : s + 128] for s in range(0, values.shape[1], 128)]
    return functools.reduce(lambda a, b: a + b, parts)


def kernel(
    keep, planes, rows_y, n_gx, n_gy, g1,
    basis, reaction, w_out, h_out,
    vecs, padded, image, react, gram_rows, proj_rows, slots1, slots2, coef,
    load_sem, last_sem, react_sem, out_sem,
    halo_send, halo_recv, send1, recv1, send2, recv2,
):
    width = basis.shape[2]
    rows = planes * rows_y
    padded_count = proj_rows.shape[1]
    gx = lax.axis_index("gx")
    gy = lax.axis_index("gy")
    n1 = n_gy * g1
    n2 = n_gx // g1
    low = lax.rem(gx, g1)
    high = gx // g1
    me1 = gy * g1 + low
    me2 = high
    cells = float(rows * width * n_gx * n_gy)

    last_copies = [
        pltpu.make_async_copy(
            basis.at[keep - 1, p * rows_y : (p + 1) * rows_y],
            padded.at[0, p + 2, 8 : rows_y + 8],
            last_sem.at[p],
        )
        for p in range(planes)
    ]
    for copy in last_copies:
        copy.start()
    bounds = [(g * keep // LOADS, (g + 1) * keep // LOADS) for g in range(LOADS)]
    loads = [
        pltpu.make_async_copy(basis.at[a:b], vecs.at[a:b], load_sem.at[g])
        for g, (a, b) in enumerate(bounds)
    ]
    for copy in loads:
        copy.start()
    react_copy = pltpu.make_async_copy(reaction, react, react_sem)
    react_copy.start()

    has_xl, has_xh = gx > 0, gx < n_gx - 1
    has_yl, has_yh = gy > 0, gy < n_gy - 1

    def member1(d):
        p = lax.rem(me1 + d, n1)
        return p, {"gx": high * g1 + lax.rem(p, g1), "gy": p // g1}

    def member2(d):
        p = lax.rem(me2 + d, n2)
        return p, {"gx": p * g1 + low, "gy": gy}

    barrier = pltpu.get_barrier_semaphore()
    for d in range(1, n1):
        pl.semaphore_signal(barrier, inc=1, device_id=member1(d)[1], device_id_type=MESH)
    for d in range(1, n2):
        pl.semaphore_signal(barrier, inc=1, device_id=member2(d)[1], device_id_type=MESH)
    sides = (
        (has_xh, {"gx": gx + 1, "gy": gy}),
        (has_xl, {"gx": gx - 1, "gy": gy}),
        (has_yh, {"gx": gx, "gy": gy + 1}),
        (has_yl, {"gx": gx, "gy": gy - 1}),
    )
    expected = n1 - 1 + n2 - 1
    for there, device in sides:
        @pl.when(there)
        def _(device=device):
            pl.semaphore_signal(barrier, inc=1, device_id=device, device_id_type=MESH)

        expected = expected + there.astype(jnp.int32)

    zero_plane = jnp.zeros((1, rows_y, width), jnp.float32)
    zero_rows = jnp.zeros((planes, 8, width), jnp.float32)
    for step in range(STEPS):
        @pl.when(jnp.logical_not(has_xl))
        def _(step=step):
            padded[step, 0:1, 8 : rows_y + 8] = zero_plane
            padded[step, 1:2, 8 : rows_y + 8] = zero_plane

        @pl.when(jnp.logical_not(has_xh))
        def _(step=step):
            padded[step, planes + 2 : planes + 3, 8 : rows_y + 8] = zero_plane

        @pl.when(jnp.logical_not(has_yl))
        def _(step=step):
            padded[step, 2 : planes + 2, 0:8] = zero_rows

        @pl.when(jnp.logical_not(has_yh))
        def _(step=step):
            padded[step, 2 : planes + 2, rows_y + 8 : rows_y + 16] = zero_rows

    gram_rows[...] = jnp.zeros(gram_rows.shape, jnp.float32)
    proj_rows[...] = jnp.zeros(proj_rows.shape, jnp.float32)
    pl.semaphore_wait(barrier, expected)

    def halo_copies(step):
        own = pl.ds(2, planes)
        refs = (
            (padded.at[step, planes : planes + 2, 8 : rows_y + 8], padded.at[step, 0:2, 8 : rows_y + 8]),
            (padded.at[step, 2:3, 8 : rows_y + 8], padded.at[step, planes + 2 : planes + 3, 8 : rows_y + 8]),
            (padded.at[step, own, rows_y : rows_y + 8], padded.at[step, own, 0:8]),
            (padded.at[step, own, 8:16], padded.at[step, own, rows_y + 8 : rows_y + 16]),
        )
        return [
            pltpu.make_async_remote_copy(
                src_ref=src, dst_ref=dst,
                send_sem=halo_send.at[step, n], recv_sem=halo_recv.at[step, n],
                device_id=sides[n][1], device_id_type=MESH,
            )
            for n, (src, dst) in enumerate(refs)
        ]

    def start_halo(step):
        for n, copy in enumerate(halo_copies(step)):
            @pl.when(sides[n][0])
            def _(copy=copy):
                copy.start()

    def wait_halo(step):
        copies = halo_copies(step)
        arrives = (has_xl, has_xh, has_yl, has_yh)
        for n, copy in enumerate(copies):
            @pl.when(arrives[n])
            def _(copy=copy):
                copy.wait_recv()

            @pl.when(sides[n][0])
            def _(copy=copy):
                copy.wait_send()

    def exchange(rnd, slots, me, count, member, send, recv, start, stop):
        def copy_of(slot, d):
            return pltpu.make_async_remote_copy(
                src_ref=slots.at[rnd, slot, start:stop], dst_ref=slots.at[rnd, slot, start:stop],
                send_sem=send.at[rnd, d - 1], recv_sem=recv.at[rnd, slot],
                device_id=member(d)[1], device_id_type=MESH,
            )

        for d in range(1, count):
            copy_of(me, d).start()
        for d in range(1, count):
            copy_of(member(d)[0], d).wait_recv()
        for d in range(1, count):
            copy_of(me, d).wait_send()
        total = slots[rnd, 0, start:stop]
        for slot in range(1, count):
            total = total + slots[rnd, slot, start:stop]
        return total

    def all_sum(rnd, start, stop):
        total = exchange(rnd, slots1, me1, n1, member1, send1, recv1, start, stop)
        if n2 > 1:
            slots2[rnd, me2, start:stop] = total
            total = exchange(rnd, slots2, me2, n2, member2, send2, recv2, start, stop)
        return total / cells

    shape = (padded_count, 128)
    lane = lax.broadcasted_iota(jnp.int32, shape, 1)
    sub = lax.broadcasted_iota(jnp.int32, shape, 0)
    eye = lane == sub
    sub8 = lax.broadcasted_iota(jnp.int32, (8, 128), 0)

    def lane_sum(values):
        return jnp.broadcast_to(jnp.sum(values, axis=1, keepdims=True), values.shape)

    def to_column(row):
        return lane_sum(jnp.where(eye, jnp.broadcast_to(row, shape), 0.0))

    def to_row(column):
        return jnp.sum(jnp.where(eye, column, 0.0), axis=0, keepdims=True)

    def project(load, count, kind):
        for first in range(0, count, 20):
            group = range(first, min(first + 20, count))

            def step(r, sums):
                at = pl.ds(pl.multiple_of(r * 8, 8), 8)
                other = load(at)
                return tuple(
                    acc + fold_lanes(vecs[i, at, :] * other) for i, acc in zip(group, sums)
                )

            zero = jnp.zeros((8, 128), jnp.float32)
            sums = lax.fori_loop(0, rows // 8, step, (zero,) * len(group))
            for i, acc in zip(group, sums):
                proj_rows[kind, i : i + 1, :] = jnp.sum(acc, axis=0, keepdims=True)

    def stencil(step):
        tall = 16
        lanes = lax.broadcasted_iota(jnp.int32, (tall, width), 1)
        sx, sy, sz = WIND_SPEEDS
        centre = 6.0 + 1.5 * (sx + sy + sz)

        def piece(p, q):
            base = pl.multiple_of(q * tall, 8)
            at = pl.ds(pl.multiple_of(base + 8, 8), tall)
            block = padded[step, p + 2, pl.ds(base, tall + 16), :]
            here = block[8 : tall + 8]
            out_at = pl.ds(pl.multiple_of(p * rows_y + base, 8), tall)
            total = -(react[out_at, :] + centre) * here
            total = total + padded[step, p + 3, at, :]
            total = total + (1.0 + 2.0 * sx) * padded[step, p + 1, at, :]
            total = total - (0.5 * sx) * padded[step, p, at, :]
            total = total + roll(block, tall + 15, 0)[8 : tall + 8]
            total = total + (1.0 + 2.0 * sy) * roll(block, 1, 0)[8 : tall + 8]
            total = total - (0.5 * sy) * roll(block, 2, 0)[8 : tall + 8]
            total = total + jnp.where(lanes < width - 1, roll(here, width - 1, 1), 0.0)
            total = total + (1.0 + 2.0 * sz) * jnp.where(lanes >= 1, roll(here, 1, 1), 0.0)
            total = total - (0.5 * sz) * jnp.where(lanes >= 2, roll(here, 2, 1), 0.0)
            image[out_at, :] = total

        @pl.loop(0, planes)
        def _(p):
            @pl.loop(0, rows_y // tall)
            def _(q):
                piece(p, q)

    def combine(step, count, scale):
        tall = 16
        scale_row = jnp.concatenate([scale] * (width // 128), axis=1)

        @pl.loop(0, planes)
        def _(p):
            @pl.loop(0, rows_y // tall)
            def _(q):
                at = pl.ds(pl.multiple_of(p * rows_y + q * tall, 8), tall)
                total = image[at, :] * scale_row
                for i in range(count):
                    total = total - coef[i : i + 1, :] * vecs[i, at, :]
                vecs[keep + step, at, :] = total
                if step < STEPS - 1:
                    padded[step + 1, p + 2, pl.ds(pl.multiple_of(q * tall + 8, 8), tall), :] = total

    def send_row(rnd, a_row, b_row):
        slots1[rnd, me1, padded_count : padded_count + 8] = jnp.where(
            sub8 == 0, a_row, jnp.where(sub8 == 1, b_row, 0.0)
        )

    for copy in last_copies:
        copy.wait()
    start_halo(0)
    ready = 0
    blocks = [(s, min(s + BLOCK, keep)) for s in range(0, keep, BLOCK)]
    for jb in range(len(blocks)):
        while ready < LOADS and bounds[ready][0] < blocks[jb][1]:
            loads[ready].wait()
            ready += 1
        for ib in range(jb + 1):
            pairs = [
                (i, j)
                for i in range(*blocks[ib])
                for j in range(*blocks[jb])
                if i <= j
            ]

            def step(r, sums, ib=ib, jb=jb, pairs=pairs):
                at = pl.ds(pl.multiple_of(r * 8, 8), 8)
                for s in range(0, width, 128):
                    needed = sorted(set(range(*blocks[ib])) | set(range(*blocks[jb])))
                    held = {i: vecs[i, at, s : s + 128] for i in needed}
                    sums = tuple(acc + held[i] * held[j] for (i, j), acc in zip(pairs, sums))
                return sums

            zero = jnp.zeros((8, 128), jnp.float32)
            sums = lax.fori_loop(0, rows // 8, step, (zero,) * len(pairs))
            for (i, j), acc in zip(pairs, sums):
                line = jnp.sum(acc, axis=0, keepdims=True)
                gram_rows[i, j : j + 1, :] = line
                if i != j:
                    gram_rows[j, i : i + 1, :] = line
    local_gram = jnp.zeros(shape, jnp.float32)
    for i in range(keep):
        local_gram = jnp.where(lane == i, lane_sum(gram_rows[i]), local_gram)
    slots1[0, me1, 0:padded_count] = local_gram
    react_copy.wait()

    gram = None
    scales = jnp.ones(shape, jnp.float32)
    hess = jnp.zeros(shape, jnp.float32)
    b_row = jnp.zeros((1, 128), jnp.float32)
    out_copies = []
    for step in range(STEPS):
        count = keep + step
        last = count - 1
        if step > 0:
            project(lambda at: vecs[last, at, :], count, 1)
            b_row = to_row(lane_sum(proj_rows[1]))
        wait_halo(step)
        stencil(step)
        project(lambda at: image[at, :], count, 0)
        send_row(step, to_row(lane_sum(proj_rows[0])), b_row)
        if step == 0:
            total = all_sum(0, 0, padded_count + 8)
            gram = total[0:padded_count]
            total = total[padded_count:]
            scale = jnp.ones((1, 128), jnp.float32)
        else:
            total = all_sum(step, padded_count, padded_count + 8)
            overlap = to_column(total[1:2])
            norm = jnp.sqrt(overlap[last : last + 1] + EPSILON)
            scale = 1.0 / norm
            hess = jnp.where((lane == step - 1) & (sub == last), norm, hess)
            scales = jnp.where(sub == last, scale, scales)
            column = jnp.where(sub < count, overlap * scales * scale, 0.0)
            gram = jnp.where(sub == last, to_row(column), gram)
            gram = jnp.where(lane == last, column, gram)
        first = jnp.where(sub < count, to_column(total[0:1]) * scales * scale, 0.0)
        weights = first + (first - lane_sum(gram * to_row(first)))
        weights = jnp.where(sub < count, weights, 0.0)
        hess = jnp.where((lane == step) & (sub < count), weights, hess)
        scaled = weights * scales
        coef[...] = jnp.concatenate([scaled] * (width // 128), axis=1)
        combine(step, count, scale)
        if step < STEPS - 1:
            start_halo(step + 1)
        copy = pltpu.make_async_copy(vecs.at[keep + step], w_out.at[step], out_sem.at[step])
        copy.start()
        out_copies.append(copy)

    last = keep + STEPS - 1

    def square(r, acc):
        values = vecs[last, pl.ds(pl.multiple_of(r * 8, 8), 8), :]
        return acc + fold_lanes(values * values)

    acc = lax.fori_loop(0, rows // 8, square, jnp.zeros((8, 128), jnp.float32))
    line = lane_sum(jnp.sum(acc, axis=0, keepdims=True))
    send_row(STEPS, line, line)
    total = all_sum(STEPS, padded_count, padded_count + 8)
    norm = jnp.sqrt(total[0:1] + EPSILON)
    hess = jnp.where((lane == STEPS - 1) & (sub == last), norm, hess)
    h_out[...] = hess
    for copy in out_copies:
        copy.wait()


def group_of(count):
    for size in (4, 2):
        if count % size == 0:
            return size
    return 1


def body(basis_vectors, reaction):
    keep, planes, rows_y, width = basis_vectors.shape
    n_gx, n_gy = lax.axis_size("gx"), lax.axis_size("gy")
    g1 = group_of(n_gx)
    n1, n2 = g1 * n_gy, n_gx // g1
    size = keep + STEPS
    padded_count = -(-size // 8) * 8
    rows = planes * rows_y
    rounds = STEPS + 1
    f32 = jnp.float32
    dma = pltpu.SemaphoreType.DMA
    w, h = pl.pallas_call(
        functools.partial(kernel, keep, planes, rows_y, n_gx, n_gy, g1),
        out_shape=(
            jax.ShapeDtypeStruct((STEPS, rows, width), f32),
            jax.ShapeDtypeStruct((padded_count, 128), f32),
        ),
        in_specs=[pl.BlockSpec(memory_space=pl.ANY)] * 2,
        out_specs=(
            pl.BlockSpec(memory_space=pl.ANY),
            pl.BlockSpec(memory_space=pltpu.VMEM),
        ),
        scratch_shapes=[
            pltpu.VMEM((size, rows, width), f32),
            pltpu.VMEM((STEPS, planes + 3, rows_y + 16, width), f32),
            pltpu.VMEM((rows, width), f32),
            pltpu.VMEM((rows, width), f32),
            pltpu.VMEM((keep, padded_count, 128), f32),
            pltpu.VMEM((2, padded_count, 128), f32),
            pltpu.VMEM((rounds, n1, padded_count + 8, 128), f32),
            pltpu.VMEM((rounds, n2, padded_count + 8, 128), f32),
            pltpu.VMEM((padded_count, width), f32),
            dma((LOADS,)),
            dma((planes,)),
            dma,
            dma((STEPS,)),
            dma((STEPS, 4)),
            dma((STEPS, 4)),
            dma((rounds, n1)),
            dma((rounds, n1)),
            dma((rounds, n2)),
            dma((rounds, n2)),
        ],
        compiler_params=pltpu.CompilerParams(
            collective_id=0, has_side_effects=True, vmem_limit_bytes=48 * 1024 * 1024
        ),
    )(basis_vectors.reshape(keep, rows, width), reaction.reshape(rows, width))
    norms = jnp.stack([h[keep + j, j] for j in range(STEPS)])
    vectors = w / norms[:, None, None]
    return vectors.reshape(STEPS, planes, rows_y, width), h[:size, :STEPS]


def solution(mesh):
    in_specs = (P(None, "gx", "gy", None), P("gx", "gy", None))
    out_specs = (P(None, "gx", "gy", None), P())
    return jax.shard_map(body, mesh=mesh, in_specs=in_specs, out_specs=out_specs, check_vma=False)
```

```python
import functools

import jax
import jax.numpy as jnp
from jax import lax
from jax.experimental import pallas as pl
from jax.experimental.pallas import tpu as pltpu
from jax.sharding import PartitionSpec as P

STEPS = 4
WIND_SPEEDS = (0.9, 0.6, 0.4)
EPSILON = 1e-06
MESH = pl.DeviceIdType.MESH
BLOCK = 6
LOADS = 6


def roll(values, shift, axis):
    return pltpu.roll(values, shift, axis)


def fold_lanes(values):
    parts = [values[:, s : s + 128] for s in range(0, values.shape[1], 128)]
    return functools.reduce(lambda a, b: a + b, parts)


def kernel(
    keep, planes, rows_y, n_gx, n_gy, g1,
    basis, reaction, w_out, h_out,
    vecs, padded, image, react, gram_rows, proj_rows, slots1, slots2, coef,
    load_sem, last_sem, react_sem, out_sem,
    halo_send, halo_recv, send1, recv1, send2, recv2,
):
    width = basis.shape[2]
    rows = planes * rows_y
    padded_count = proj_rows.shape[1]
    gx = lax.axis_index("gx")
    gy = lax.axis_index("gy")
    n1 = n_gy * g1
    n2 = n_gx // g1
    low = lax.rem(gx, g1)
    high = gx // g1
    me1 = gy * g1 + low
    me2 = high
    cells = float(rows * width * n_gx * n_gy)

    last_copies = [
        pltpu.make_async_copy(
            basis.at[keep - 1, p * rows_y : (p + 1) * rows_y],
            padded.at[0, p + 2, 8 : rows_y + 8],
            last_sem.at[p],
        )
        for p in range(planes)
    ]
    for copy in last_copies:
        copy.start()
    bounds = [(g * keep // LOADS, (g + 1) * keep // LOADS) for g in range(LOADS)]
    loads = [
        pltpu.make_async_copy(basis.at[a:b], vecs.at[a:b], load_sem.at[g])
        for g, (a, b) in enumerate(bounds)
    ]
    for copy in loads:
        copy.start()
    react_copy = pltpu.make_async_copy(reaction, react, react_sem)
    react_copy.start()

    has_xl, has_xh = gx > 0, gx < n_gx - 1
    has_yl, has_yh = gy > 0, gy < n_gy - 1

    def member1(d):
        p = lax.rem(me1 + d, n1)
        return p, {"gx": high * g1 + lax.rem(p, g1), "gy": p // g1}

    def member2(d):
        p = lax.rem(me2 + d, n2)
        return p, {"gx": p * g1 + low, "gy": gy}

    barrier = pltpu.get_barrier_semaphore()
    for d in range(1, n1):
        pl.semaphore_signal(barrier, inc=1, device_id=member1(d)[1], device_id_type=MESH)
    for d in range(1, n2):
        pl.semaphore_signal(barrier, inc=1, device_id=member2(d)[1], device_id_type=MESH)
    sides = (
        (has_xh, {"gx": gx + 1, "gy": gy}),
        (has_xl, {"gx": gx - 1, "gy": gy}),
        (has_yh, {"gx": gx, "gy": gy + 1}),
        (has_yl, {"gx": gx, "gy": gy - 1}),
    )
    expected = n1 - 1 + n2 - 1
    for there, device in sides:
        @pl.when(there)
        def _(device=device):
            pl.semaphore_signal(barrier, inc=1, device_id=device, device_id_type=MESH)

        expected = expected + there.astype(jnp.int32)

    zero_plane = jnp.zeros((1, rows_y, width), jnp.float32)
    zero_rows = jnp.zeros((planes, 8, width), jnp.float32)
    for step in range(STEPS):
        @pl.when(jnp.logical_not(has_xl))
        def _(step=step):
            padded[step, 0:1, 8 : rows_y + 8] = zero_plane
            padded[step, 1:2, 8 : rows_y + 8] = zero_plane

        @pl.when(jnp.logical_not(has_xh))
        def _(step=step):
            padded[step, planes + 2 : planes + 3, 8 : rows_y + 8] = zero_plane

        @pl.when(jnp.logical_not(has_yl))
        def _(step=step):
            padded[step, 2 : planes + 2, 0:8] = zero_rows

        @pl.when(jnp.logical_not(has_yh))
        def _(step=step):
            padded[step, 2 : planes + 2, rows_y + 8 : rows_y + 16] = zero_rows

    gram_rows[...] = jnp.zeros(gram_rows.shape, jnp.float32)
    proj_rows[...] = jnp.zeros(proj_rows.shape, jnp.float32)
    pl.semaphore_wait(barrier, expected)

    def halo_copies(step):
        own = pl.ds(2, planes)
        refs = (
            (padded.at[step, planes : planes + 2, 8 : rows_y + 8], padded.at[step, 0:2, 8 : rows_y + 8]),
            (padded.at[step, 2:3, 8 : rows_y + 8], padded.at[step, planes + 2 : planes + 3, 8 : rows_y + 8]),
            (padded.at[step, own, rows_y : rows_y + 8], padded.at[step, own, 0:8]),
            (padded.at[step, own, 8:16], padded.at[step, own, rows_y + 8 : rows_y + 16]),
        )
        return [
            pltpu.make_async_remote_copy(
                src_ref=src, dst_ref=dst,
                send_sem=halo_send.at[step, n], recv_sem=halo_recv.at[step, n],
                device_id=sides[n][1], device_id_type=MESH,
            )
            for n, (src, dst) in enumerate(refs)
        ]

    def start_halo(step, which):
        copies = halo_copies(step)
        for n in which:
            copy = copies[n]

            @pl.when(sides[n][0])
            def _(copy=copy):
                copy.start()

    def wait_halo(step, which):
        copies = halo_copies(step)
        arrives = (has_xl, has_xh, has_yl, has_yh)
        for n in which:
            copy = copies[n]

            @pl.when(arrives[n])
            def _(copy=copy):
                copy.wait_recv()

            @pl.when(sides[n][0])
            def _(copy=copy):
                copy.wait_send()

    stage1 = (slots1, me1, n1, member1, send1, recv1)
    stage2 = (slots2, me2, n2, member2, send2, recv2)

    def exchange(rnd, stage, start, stop, begin):
        slots, me, count, member, send, recv = stage

        def copy_of(slot, d):
            return pltpu.make_async_remote_copy(
                src_ref=slots.at[rnd, slot, start:stop], dst_ref=slots.at[rnd, slot, start:stop],
                send_sem=send.at[rnd, d - 1], recv_sem=recv.at[rnd, slot],
                device_id=member(d)[1], device_id_type=MESH,
            )

        if begin:
            for d in range(1, count):
                copy_of(me, d).start()
            return None
        for d in range(1, count):
            copy_of(member(d)[0], d).wait_recv()
        for d in range(1, count):
            copy_of(me, d).wait_send()
        total = slots[rnd, 0, start:stop]
        for slot in range(1, count):
            total = total + slots[rnd, slot, start:stop]
        return total

    def begin1(rnd, start, stop):
        exchange(rnd, stage1, start, stop, True)

    def begin2(rnd, start, stop):
        slots2[rnd, me2, start:stop] = exchange(rnd, stage1, start, stop, False)
        exchange(rnd, stage2, start, stop, True)

    def finish(rnd, start, stop):
        return exchange(rnd, stage2, start, stop, False) / cells

    def all_sum(rnd, start, stop):
        begin1(rnd, start, stop)
        begin2(rnd, start, stop)
        return finish(rnd, start, stop)

    shape = (padded_count, 128)
    lane = lax.broadcasted_iota(jnp.int32, shape, 1)
    sub = lax.broadcasted_iota(jnp.int32, shape, 0)
    eye = lane == sub
    sub8 = lax.broadcasted_iota(jnp.int32, (8, 128), 0)

    def lane_sum(values):
        return jnp.broadcast_to(jnp.sum(values, axis=1, keepdims=True), values.shape)

    def to_column(row):
        return lane_sum(jnp.where(eye, jnp.broadcast_to(row, shape), 0.0))

    def to_row(column):
        return jnp.sum(jnp.where(eye, column, 0.0), axis=0, keepdims=True)

    def project(load, count, kind):
        for first in range(0, count, 20):
            group = range(first, min(first + 20, count))

            def step(r, sums):
                at = pl.ds(pl.multiple_of(r * 8, 8), 8)
                other = load(at)
                return tuple(
                    acc + fold_lanes(vecs[i, at, :] * other) for i, acc in zip(group, sums)
                )

            zero = jnp.zeros((8, 128), jnp.float32)
            sums = lax.fori_loop(0, rows // 8, step, (zero,) * len(group))
            for i, acc in zip(group, sums):
                proj_rows[kind, i : i + 1, :] = jnp.sum(acc, axis=0, keepdims=True)

    def stencil(step):
        tall = 16
        lanes = lax.broadcasted_iota(jnp.int32, (tall, width), 1)
        sx, sy, sz = WIND_SPEEDS
        centre = 6.0 + 1.5 * (sx + sy + sz)

        def piece(p, q):
            base = pl.multiple_of(q * tall, 8)
            at = pl.ds(pl.multiple_of(base + 8, 8), tall)
            block = padded[step, p + 2, pl.ds(base, tall + 16), :]
            here = block[8 : tall + 8]
            out_at = pl.ds(pl.multiple_of(p * rows_y + base, 8), tall)
            total = -(react[out_at, :] + centre) * here
            total = total + padded[step, p + 3, at, :]
            total = total + (1.0 + 2.0 * sx) * padded[step, p + 1, at, :]
            total = total - (0.5 * sx) * padded[step, p, at, :]
            total = total + roll(block, tall + 15, 0)[8 : tall + 8]
            total = total + (1.0 + 2.0 * sy) * roll(block, 1, 0)[8 : tall + 8]
            total = total - (0.5 * sy) * roll(block, 2, 0)[8 : tall + 8]
            total = total + jnp.where(lanes < width - 1, roll(here, width - 1, 1), 0.0)
            total = total + (1.0 + 2.0 * sz) * jnp.where(lanes >= 1, roll(here, 1, 1), 0.0)
            total = total - (0.5 * sz) * jnp.where(lanes >= 2, roll(here, 2, 1), 0.0)
            image[out_at, :] = total

        inner = range(2, planes - 1)
        wait_halo(step, (2, 3))
        for p in inner:
            @pl.loop(0, rows_y // tall)
            def _(q, p=p):
                piece(p, q)

        wait_halo(step, (0, 1))
        for p in [p for p in range(planes) if p not in inner]:
            @pl.loop(0, rows_y // tall)
            def _(q, p=p):
                piece(p, q)

    def combine(step, count, scale):
        tall = 32 if rows_y % 32 == 0 else 16
        scale_row = jnp.concatenate([scale] * (width // 128), axis=1)

        def plane(p):
            @pl.loop(0, rows_y // tall)
            def _(q):
                at = pl.ds(pl.multiple_of(p * rows_y + q * tall, 8), tall)
                total = image[at, :] * scale_row
                for i in range(count):
                    total = total - coef[i : i + 1, :] * vecs[i, at, :]
                vecs[keep + step, at, :] = total
                if step < STEPS - 1:
                    padded[step + 1, p + 2, pl.ds(pl.multiple_of(q * tall + 8, 8), tall), :] = total

        more = step < STEPS - 1
        done = []
        for part, side in (((planes - 2, planes - 1), 0), ((0,), 1), (range(planes), 2)):
            for p in part:
                if p not in done:
                    plane(p)
                    done.append(p)
            if more:
                start_halo(step + 1, (side,) if side < 2 else (2, 3))

    def send_row(rnd, a_row, b_row):
        slots1[rnd, me1, padded_count : padded_count + 8] = jnp.where(
            sub8 == 0, a_row, jnp.where(sub8 == 1, b_row, 0.0)
        )

    for copy in last_copies:
        copy.wait()
    start_halo(0, (0, 1, 2, 3))
    ready = 0
    blocks = [(s, min(s + BLOCK, keep)) for s in range(0, keep, BLOCK)]
    for jb in range(len(blocks)):
        while ready < LOADS and bounds[ready][0] < blocks[jb][1]:
            loads[ready].wait()
            ready += 1
        for ib in range(jb + 1):
            pairs = [
                (i, j)
                for i in range(*blocks[ib])
                for j in range(*blocks[jb])
                if i <= j
            ]

            def step(r, sums, ib=ib, jb=jb, pairs=pairs):
                at = pl.ds(pl.multiple_of(r * 8, 8), 8)
                for s in range(0, width, 128):
                    needed = sorted(set(range(*blocks[ib])) | set(range(*blocks[jb])))
                    held = {i: vecs[i, at, s : s + 128] for i in needed}
                    sums = tuple(acc + held[i] * held[j] for (i, j), acc in zip(pairs, sums))
                return sums

            zero = jnp.zeros((8, 128), jnp.float32)
            sums = lax.fori_loop(0, rows // 8, step, (zero,) * len(pairs))
            for (i, j), acc in zip(pairs, sums):
                line = jnp.sum(acc, axis=0, keepdims=True)
                gram_rows[i, j : j + 1, :] = line
                if i != j:
                    gram_rows[j, i : i + 1, :] = line
    local_gram = jnp.zeros(shape, jnp.float32)
    for i in range(keep):
        local_gram = jnp.where(lane == i, lane_sum(gram_rows[i]), local_gram)
    slots1[STEPS + 1, me1, 0:padded_count] = local_gram
    react_copy.wait()
    begin1(STEPS + 1, 0, padded_count)

    gram = None
    scales = jnp.ones(shape, jnp.float32)
    hess = jnp.zeros(shape, jnp.float32)
    b_row = jnp.zeros((1, 128), jnp.float32)
    out_copies = []
    for step in range(STEPS):
        count = keep + step
        last = count - 1
        if step > 0:
            project(lambda at: vecs[last, at, :], count, 1)
            b_row = to_row(lane_sum(proj_rows[1]))
        stencil(step)
        project(lambda at: image[at, :], count, 0)
        send_row(step, to_row(lane_sum(proj_rows[0])), b_row)
        if step == 0:
            begin1(0, padded_count, padded_count + 8)
            begin2(STEPS + 1, 0, padded_count)
            begin2(0, padded_count, padded_count + 8)
            gram = finish(STEPS + 1, 0, padded_count)
            total = finish(0, padded_count, padded_count + 8)
            scale = jnp.ones((1, 128), jnp.float32)
        else:
            total = all_sum(step, padded_count, padded_count + 8)
            overlap = to_column(total[1:2])
            norm = jnp.sqrt(overlap[last : last + 1] + EPSILON)
            scale = 1.0 / norm
            hess = jnp.where((lane == step - 1) & (sub == last), norm, hess)
            scales = jnp.where(sub == last, scale, scales)
            column = jnp.where(sub < count, overlap * scales * scale, 0.0)
            gram = jnp.where(sub == last, to_row(column), gram)
            gram = jnp.where(lane == last, column, gram)
        first = jnp.where(sub < count, to_column(total[0:1]) * scales * scale, 0.0)
        weights = first + (first - lane_sum(gram * to_row(first)))
        weights = jnp.where(sub < count, weights, 0.0)
        hess = jnp.where((lane == step) & (sub < count), weights, hess)
        scaled = weights * scales
        coef[...] = jnp.concatenate([scaled] * (width // 128), axis=1)
        combine(step, count, scale)
        copy = pltpu.make_async_copy(vecs.at[keep + step], w_out.at[step], out_sem.at[step])
        copy.start()
        out_copies.append(copy)

    last = keep + STEPS - 1

    def square(r, acc):
        values = vecs[last, pl.ds(pl.multiple_of(r * 8, 8), 8), :]
        return acc + fold_lanes(values * values)

    acc = lax.fori_loop(0, rows // 8, square, jnp.zeros((8, 128), jnp.float32))
    line = lane_sum(jnp.sum(acc, axis=0, keepdims=True))
    send_row(STEPS, line, line)
    total = all_sum(STEPS, padded_count, padded_count + 8)
    norm = jnp.sqrt(total[0:1] + EPSILON)
    hess = jnp.where((lane == STEPS - 1) & (sub == last), norm, hess)
    h_out[...] = hess
    for copy in out_copies:
        copy.wait()


def group_of(count):
    for size in (4, 2):
        if count % size == 0:
            return size
    return 1


def body(basis_vectors, reaction):
    keep, planes, rows_y, width = basis_vectors.shape
    n_gx, n_gy = lax.axis_size("gx"), lax.axis_size("gy")
    g1 = group_of(n_gx)
    n1, n2 = g1 * n_gy, n_gx // g1
    size = keep + STEPS
    padded_count = -(-size // 8) * 8
    rows = planes * rows_y
    rounds = STEPS + 2
    f32 = jnp.float32
    dma = pltpu.SemaphoreType.DMA
    w, h = pl.pallas_call(
        functools.partial(kernel, keep, planes, rows_y, n_gx, n_gy, g1),
        out_shape=(
            jax.ShapeDtypeStruct((STEPS, rows, width), f32),
            jax.ShapeDtypeStruct((padded_count, 128), f32),
        ),
        in_specs=[pl.BlockSpec(memory_space=pl.ANY)] * 2,
        out_specs=(
            pl.BlockSpec(memory_space=pl.ANY),
            pl.BlockSpec(memory_space=pltpu.VMEM),
        ),
        scratch_shapes=[
            pltpu.VMEM((size, rows, width), f32),
            pltpu.VMEM((STEPS, planes + 3, rows_y + 16, width), f32),
            pltpu.VMEM((rows, width), f32),
            pltpu.VMEM((rows, width), f32),
            pltpu.VMEM((keep, padded_count, 128), f32),
            pltpu.VMEM((2, padded_count, 128), f32),
            pltpu.VMEM((rounds, n1, padded_count + 8, 128), f32),
            pltpu.VMEM((rounds, n2, padded_count + 8, 128), f32),
            pltpu.VMEM((padded_count, width), f32),
            dma((LOADS,)),
            dma((planes,)),
            dma,
            dma((STEPS,)),
            dma((STEPS, 4)),
            dma((STEPS, 4)),
            dma((rounds, n1)),
            dma((rounds, n1)),
            dma((rounds, n2)),
            dma((rounds, n2)),
        ],
        compiler_params=pltpu.CompilerParams(
            collective_id=0, has_side_effects=True, vmem_limit_bytes=48 * 1024 * 1024
        ),
    )(basis_vectors.reshape(keep, rows, width), reaction.reshape(rows, width))
    norms = jnp.stack([h[keep + j, j] for j in range(STEPS)])
    vectors = w / norms[:, None, None]
    return vectors.reshape(STEPS, planes, rows_y, width), h[:size, :STEPS]


def solution(mesh):
    in_specs = (P(None, "gx", "gy", None), P("gx", "gy", None))
    out_specs = (P(None, "gx", "gy", None), P())
    return jax.shard_map(body, mesh=mesh, in_specs=in_specs, out_specs=out_specs, check_vma=False)
```

```python
import functools

import jax
import jax.numpy as jnp
from jax import lax
from jax.experimental import pallas as pl
from jax.experimental.pallas import tpu as pltpu
from jax.sharding import PartitionSpec as P

STEPS = 4
WIND_SPEEDS = (0.9, 0.6, 0.4)
EPSILON = 1e-06
MESH = pl.DeviceIdType.MESH
BLOCK = 6
LOADS = 6


def roll(values, shift, axis):
    return pltpu.roll(values, shift, axis)


def fold_lanes(values):
    parts = [values[:, s : s + 128] for s in range(0, values.shape[1], 128)]
    return functools.reduce(lambda a, b: a + b, parts)


def kernel(
    keep, planes, rows_y, n_gx, n_gy, g1,
    basis, reaction, w_out, h_out,
    vecs, padded, image, react, gram_rows, proj_rows, slots1, slots2, coef,
    load_sem, last_sem, react_sem, out_sem,
    halo_send, halo_recv, send1, recv1, send2, recv2,
):
    width = basis.shape[2]
    rows = planes * rows_y
    padded_count = proj_rows.shape[1]
    gx = lax.axis_index("gx")
    gy = lax.axis_index("gy")
    n1 = n_gy * g1
    n2 = n_gx // g1
    low = lax.rem(gx, g1)
    high = gx // g1
    me1 = gy * g1 + low
    me2 = high
    cells = float(rows * width * n_gx * n_gy)

    last_copies = [
        pltpu.make_async_copy(
            basis.at[keep - 1, p * rows_y : (p + 1) * rows_y],
            padded.at[0, p + 2, 8 : rows_y + 8],
            last_sem.at[p],
        )
        for p in range(planes)
    ]
    for copy in last_copies:
        copy.start()
    bounds = [(g * keep // LOADS, (g + 1) * keep // LOADS) for g in range(LOADS)]
    loads = [
        pltpu.make_async_copy(basis.at[a:b], vecs.at[a:b], load_sem.at[g])
        for g, (a, b) in enumerate(bounds)
    ]
    for copy in loads:
        copy.start()
    react_copy = pltpu.make_async_copy(reaction, react, react_sem)
    react_copy.start()

    has_xl, has_xh = gx > 0, gx < n_gx - 1
    has_yl, has_yh = gy > 0, gy < n_gy - 1

    def member1(d):
        p = lax.rem(me1 + d, n1)
        return p, {"gx": high * g1 + lax.rem(p, g1), "gy": p // g1}

    def member2(d):
        p = lax.rem(me2 + d, n2)
        return p, {"gx": p * g1 + low, "gy": gy}

    barrier = pltpu.get_barrier_semaphore()
    for d in range(1, n1):
        pl.semaphore_signal(barrier, inc=1, device_id=member1(d)[1], device_id_type=MESH)
    for d in range(1, n2):
        pl.semaphore_signal(barrier, inc=1, device_id=member2(d)[1], device_id_type=MESH)
    sides = (
        (has_xh, {"gx": gx + 1, "gy": gy}),
        (has_xl, {"gx": gx - 1, "gy": gy}),
        (has_yh, {"gx": gx, "gy": gy + 1}),
        (has_yl, {"gx": gx, "gy": gy - 1}),
    )
    expected = n1 - 1 + n2 - 1
    for there, device in sides:
        @pl.when(there)
        def _(device=device):
            pl.semaphore_signal(barrier, inc=1, device_id=device, device_id_type=MESH)

        expected = expected + there.astype(jnp.int32)

    zero_plane = jnp.zeros((1, rows_y, width), jnp.float32)
    zero_rows = jnp.zeros((planes, 8, width), jnp.float32)
    for step in range(STEPS):
        @pl.when(jnp.logical_not(has_xl))
        def _(step=step):
            padded[step, 0:1, 8 : rows_y + 8] = zero_plane
            padded[step, 1:2, 8 : rows_y + 8] = zero_plane

        @pl.when(jnp.logical_not(has_xh))
        def _(step=step):
            padded[step, planes + 2 : planes + 3, 8 : rows_y + 8] = zero_plane

        @pl.when(jnp.logical_not(has_yl))
        def _(step=step):
            padded[step, 2 : planes + 2, 0:8] = zero_rows

        @pl.when(jnp.logical_not(has_yh))
        def _(step=step):
            padded[step, 2 : planes + 2, rows_y + 8 : rows_y + 16] = zero_rows

    gram_rows[...] = jnp.zeros(gram_rows.shape, jnp.float32)
    proj_rows[...] = jnp.zeros(proj_rows.shape, jnp.float32)
    pl.semaphore_wait(barrier, expected)

    def halo_copies(step):
        own = pl.ds(2, planes)
        refs = (
            (padded.at[step, planes : planes + 2, 8 : rows_y + 8], padded.at[step, 0:2, 8 : rows_y + 8]),
            (padded.at[step, 2:3, 8 : rows_y + 8], padded.at[step, planes + 2 : planes + 3, 8 : rows_y + 8]),
            (padded.at[step, own, rows_y : rows_y + 8], padded.at[step, own, 0:8]),
            (padded.at[step, own, 8:16], padded.at[step, own, rows_y + 8 : rows_y + 16]),
        )
        return [
            pltpu.make_async_remote_copy(
                src_ref=src, dst_ref=dst,
                send_sem=halo_send.at[step, n], recv_sem=halo_recv.at[step, n],
                device_id=sides[n][1], device_id_type=MESH,
            )
            for n, (src, dst) in enumerate(refs)
        ]

    def start_halo(step, which):
        copies = halo_copies(step)
        for n in which:
            copy = copies[n]

            @pl.when(sides[n][0])
            def _(copy=copy):
                copy.start()

    def wait_halo(step, which):
        copies = halo_copies(step)
        arrives = (has_xl, has_xh, has_yl, has_yh)
        for n in which:
            copy = copies[n]

            @pl.when(arrives[n])
            def _(copy=copy):
                copy.wait_recv()

            @pl.when(sides[n][0])
            def _(copy=copy):
                copy.wait_send()

    stage1 = (slots1, me1, n1, member1, send1, recv1)
    stage2 = (slots2, me2, n2, member2, send2, recv2)

    def exchange(rnd, stage, start, stop, begin):
        slots, me, count, member, send, recv = stage

        def copy_of(slot, d):
            return pltpu.make_async_remote_copy(
                src_ref=slots.at[rnd, slot, start:stop], dst_ref=slots.at[rnd, slot, start:stop],
                send_sem=send.at[rnd, d - 1], recv_sem=recv.at[rnd, slot],
                device_id=member(d)[1], device_id_type=MESH,
            )

        if begin:
            for d in range(1, count):
                copy_of(me, d).start()
            return None
        for d in range(1, count):
            copy_of(member(d)[0], d).wait_recv()
        for d in range(1, count):
            copy_of(me, d).wait_send()
        total = slots[rnd, 0, start:stop]
        for slot in range(1, count):
            total = total + slots[rnd, slot, start:stop]
        return total

    def begin1(rnd, start, stop):
        exchange(rnd, stage1, start, stop, True)

    def begin2(rnd, start, stop):
        slots2[rnd, me2, start:stop] = exchange(rnd, stage1, start, stop, False)
        exchange(rnd, stage2, start, stop, True)

    def finish(rnd, start, stop):
        return exchange(rnd, stage2, start, stop, False) / cells

    def all_sum(rnd, start, stop):
        begin1(rnd, start, stop)
        begin2(rnd, start, stop)
        return finish(rnd, start, stop)

    shape = (padded_count, 128)
    lane = lax.broadcasted_iota(jnp.int32, shape, 1)
    sub = lax.broadcasted_iota(jnp.int32, shape, 0)
    eye = lane == sub
    sub8 = lax.broadcasted_iota(jnp.int32, (8, 128), 0)

    def lane_sum(values):
        return jnp.broadcast_to(jnp.sum(values, axis=1, keepdims=True), values.shape)

    def to_column(row):
        return lane_sum(jnp.where(eye, jnp.broadcast_to(row, shape), 0.0))

    def to_row(column):
        return jnp.sum(jnp.where(eye, column, 0.0), axis=0, keepdims=True)

    def project(load, count, kind):
        for first in range(0, count, 20):
            group = range(first, min(first + 20, count))

            def step(r, sums):
                at = pl.ds(pl.multiple_of(r * 8, 8), 8)
                other = load(at)
                return tuple(
                    acc + fold_lanes(vecs[i, at, :] * other) for i, acc in zip(group, sums)
                )

            zero = jnp.zeros((8, 128), jnp.float32)
            sums = lax.fori_loop(0, rows // 8, step, (zero,) * len(group), unroll=4)
            for i, acc in zip(group, sums):
                proj_rows[kind, i : i + 1, :] = jnp.sum(acc, axis=0, keepdims=True)

    def stencil(step):
        tall = 16
        lanes = lax.broadcasted_iota(jnp.int32, (tall, width), 1)
        sx, sy, sz = WIND_SPEEDS
        centre = 6.0 + 1.5 * (sx + sy + sz)

        def piece(p, q):
            base = pl.multiple_of(q * tall, 8)
            at = pl.ds(pl.multiple_of(base + 8, 8), tall)
            block = padded[step, p + 2, pl.ds(base, tall + 16), :]
            here = block[8 : tall + 8]
            out_at = pl.ds(pl.multiple_of(p * rows_y + base, 8), tall)
            total = -(react[out_at, :] + centre) * here
            total = total + padded[step, p + 3, at, :]
            total = total + (1.0 + 2.0 * sx) * padded[step, p + 1, at, :]
            total = total - (0.5 * sx) * padded[step, p, at, :]
            total = total + roll(block, tall + 15, 0)[8 : tall + 8]
            total = total + (1.0 + 2.0 * sy) * roll(block, 1, 0)[8 : tall + 8]
            total = total - (0.5 * sy) * roll(block, 2, 0)[8 : tall + 8]
            total = total + jnp.where(lanes < width - 1, roll(here, width - 1, 1), 0.0)
            total = total + (1.0 + 2.0 * sz) * jnp.where(lanes >= 1, roll(here, 1, 1), 0.0)
            total = total - (0.5 * sz) * jnp.where(lanes >= 2, roll(here, 2, 1), 0.0)
            image[out_at, :] = total

        inner = range(2, planes - 1)
        wait_halo(step, (2, 3))
        for p in inner:
            @pl.loop(0, rows_y // tall, unroll=True)
            def _(q, p=p):
                piece(p, q)

        wait_halo(step, (0, 1))
        for p in [p for p in range(planes) if p not in inner]:
            @pl.loop(0, rows_y // tall, unroll=True)
            def _(q, p=p):
                piece(p, q)

    def combine(step, count, scale):
        tall = 32 if rows_y % 32 == 0 else 16
        scale_row = jnp.concatenate([scale] * (width // 128), axis=1)

        def plane(p):
            @pl.loop(0, rows_y // tall)
            def _(q):
                at = pl.ds(pl.multiple_of(p * rows_y + q * tall, 8), tall)
                total = image[at, :] * scale_row
                for i in range(count):
                    total = total - coef[i : i + 1, :] * vecs[i, at, :]
                vecs[keep + step, at, :] = total
                if step < STEPS - 1:
                    padded[step + 1, p + 2, pl.ds(pl.multiple_of(q * tall + 8, 8), tall), :] = total

        more = step < STEPS - 1
        done = []
        for part, side in (((planes - 2, planes - 1), 0), ((0,), 1), (range(planes), 2)):
            for p in part:
                if p not in done:
                    plane(p)
                    done.append(p)
            if more:
                start_halo(step + 1, (side,) if side < 2 else (2, 3))

    def send_row(rnd, a_row, b_row):
        slots1[rnd, me1, padded_count : padded_count + 8] = jnp.where(
            sub8 == 0, a_row, jnp.where(sub8 == 1, b_row, 0.0)
        )

    for copy in last_copies:
        copy.wait()
    start_halo(0, (0, 1, 2, 3))
    ready = 0
    blocks = [(s, min(s + BLOCK, keep)) for s in range(0, keep, BLOCK)]
    for jb in range(len(blocks)):
        while ready < LOADS and bounds[ready][0] < blocks[jb][1]:
            loads[ready].wait()
            ready += 1
        for ib in range(jb + 1):
            pairs = [
                (i, j)
                for i in range(*blocks[ib])
                for j in range(*blocks[jb])
                if i <= j
            ]

            def step(r, sums, ib=ib, jb=jb, pairs=pairs):
                at = pl.ds(pl.multiple_of(r * 8, 8), 8)
                for s in range(0, width, 128):
                    needed = sorted(set(range(*blocks[ib])) | set(range(*blocks[jb])))
                    held = {i: vecs[i, at, s : s + 128] for i in needed}
                    sums = tuple(acc + held[i] * held[j] for (i, j), acc in zip(pairs, sums))
                return sums

            zero = jnp.zeros((8, 128), jnp.float32)
            sums = lax.fori_loop(0, rows // 8, step, (zero,) * len(pairs))
            for (i, j), acc in zip(pairs, sums):
                line = jnp.sum(acc, axis=0, keepdims=True)
                gram_rows[i, j : j + 1, :] = line
                if i != j:
                    gram_rows[j, i : i + 1, :] = line
    local_gram = jnp.zeros(shape, jnp.float32)
    for i in range(keep):
        local_gram = jnp.where(lane == i, lane_sum(gram_rows[i]), local_gram)
    slots1[STEPS + 1, me1, 0:padded_count] = local_gram
    react_copy.wait()
    begin1(STEPS + 1, 0, padded_count)

    gram = None
    scales = jnp.ones(shape, jnp.float32)
    hess = jnp.zeros(shape, jnp.float32)
    b_row = jnp.zeros((1, 128), jnp.float32)
    out_copies = []
    for step in range(STEPS):
        count = keep + step
        last = count - 1
        if step > 0:
            project(lambda at: vecs[last, at, :], count, 1)
            b_row = to_row(lane_sum(proj_rows[1]))
        stencil(step)
        project(lambda at: image[at, :], count, 0)
        send_row(step, to_row(lane_sum(proj_rows[0])), b_row)
        if step == 0:
            begin1(0, padded_count, padded_count + 8)
            begin2(STEPS + 1, 0, padded_count)
            begin2(0, padded_count, padded_count + 8)
            gram = finish(STEPS + 1, 0, padded_count)
            total = finish(0, padded_count, padded_count + 8)
            scale = jnp.ones((1, 128), jnp.float32)
        else:
            total = all_sum(step, padded_count, padded_count + 8)
            overlap = to_column(total[1:2])
            norm = jnp.sqrt(overlap[last : last + 1] + EPSILON)
            scale = 1.0 / norm
            hess = jnp.where((lane == step - 1) & (sub == last), norm, hess)
            scales = jnp.where(sub == last, scale, scales)
            column = jnp.where(sub < count, overlap * scales * scale, 0.0)
            gram = jnp.where(sub == last, to_row(column), gram)
            gram = jnp.where(lane == last, column, gram)
        first = jnp.where(sub < count, to_column(total[0:1]) * scales * scale, 0.0)
        weights = first + (first - lane_sum(gram * to_row(first)))
        weights = jnp.where(sub < count, weights, 0.0)
        hess = jnp.where((lane == step) & (sub < count), weights, hess)
        scaled = weights * scales
        coef[...] = jnp.concatenate([scaled] * (width // 128), axis=1)
        combine(step, count, scale)
        copy = pltpu.make_async_copy(vecs.at[keep + step], w_out.at[step], out_sem.at[step])
        copy.start()
        out_copies.append(copy)

    last = keep + STEPS - 1

    def square(r, acc):
        values = vecs[last, pl.ds(pl.multiple_of(r * 8, 8), 8), :]
        return acc + fold_lanes(values * values)

    acc = lax.fori_loop(0, rows // 8, square, jnp.zeros((8, 128), jnp.float32))
    line = lane_sum(jnp.sum(acc, axis=0, keepdims=True))
    send_row(STEPS, line, line)
    total = all_sum(STEPS, padded_count, padded_count + 8)
    norm = jnp.sqrt(total[0:1] + EPSILON)
    hess = jnp.where((lane == STEPS - 1) & (sub == last), norm, hess)
    h_out[...] = hess
    for copy in out_copies:
        copy.wait()


def group_of(count):
    for size in (4, 2):
        if count % size == 0:
            return size
    return 1


def body(basis_vectors, reaction):
    keep, planes, rows_y, width = basis_vectors.shape
    n_gx, n_gy = lax.axis_size("gx"), lax.axis_size("gy")
    g1 = group_of(n_gx)
    n1, n2 = g1 * n_gy, n_gx // g1
    size = keep + STEPS
    padded_count = -(-size // 8) * 8
    rows = planes * rows_y
    rounds = STEPS + 2
    f32 = jnp.float32
    dma = pltpu.SemaphoreType.DMA
    w, h = pl.pallas_call(
        functools.partial(kernel, keep, planes, rows_y, n_gx, n_gy, g1),
        out_shape=(
            jax.ShapeDtypeStruct((STEPS, rows, width), f32),
            jax.ShapeDtypeStruct((padded_count, 128), f32),
        ),
        in_specs=[pl.BlockSpec(memory_space=pl.ANY)] * 2,
        out_specs=(
            pl.BlockSpec(memory_space=pl.ANY),
            pl.BlockSpec(memory_space=pltpu.VMEM),
        ),
        scratch_shapes=[
            pltpu.VMEM((size, rows, width), f32),
            pltpu.VMEM((STEPS, planes + 3, rows_y + 16, width), f32),
            pltpu.VMEM((rows, width), f32),
            pltpu.VMEM((rows, width), f32),
            pltpu.VMEM((keep, padded_count, 128), f32),
            pltpu.VMEM((2, padded_count, 128), f32),
            pltpu.VMEM((rounds, n1, padded_count + 8, 128), f32),
            pltpu.VMEM((rounds, n2, padded_count + 8, 128), f32),
            pltpu.VMEM((padded_count, width), f32),
            dma((LOADS,)),
            dma((planes,)),
            dma,
            dma((STEPS,)),
            dma((STEPS, 4)),
            dma((STEPS, 4)),
            dma((rounds, n1)),
            dma((rounds, n1)),
            dma((rounds, n2)),
            dma((rounds, n2)),
        ],
        compiler_params=pltpu.CompilerParams(
            collective_id=0, has_side_effects=True, vmem_limit_bytes=48 * 1024 * 1024
        ),
    )(basis_vectors.reshape(keep, rows, width), reaction.reshape(rows, width))
    norms = jnp.stack([h[keep + j, j] for j in range(STEPS)])
    vectors = w / norms[:, None, None]
    return vectors.reshape(STEPS, planes, rows_y, width), h[:size, :STEPS]


def solution(mesh):
    in_specs = (P(None, "gx", "gy", None), P("gx", "gy", None))
    out_specs = (P(None, "gx", "gy", None), P())
    return jax.shard_map(body, mesh=mesh, in_specs=in_specs, out_specs=out_specs, check_vma=False)
```
